8 devices in a mesh: ens: 1 (over z), sp: 8 (over y, x, core).
Axes of the slice: x: 2, y: 2, z: 1, core: 2. Of those that a mesh axis runs over, the one named last changes fastest.
Arguments:
- x_seq: bfloat16 [8192, 256], P(('ens', 'sp'))
- w_past: bfloat16 [2, 10, 256, 512], replicated
- w_now: bfloat16 [2, 10, 256, 512], replicated
- b_conv: float32 [2, 10, 512], replicated
- w_res: bfloat16 [2, 10, 256, 256], replicated
- w_skip: bfloat16 [2, 10, 256, 256], replicated
- w_out1: bfloat16 [256, 256], replicated
- b_out1: float32 [256], replicated
- w_out2: bfloat16 [256, 256], replicated
- b_out2: float32 [256], replicated
Outputs:
- output 1: float32 [8192, 256], P(('ens', 'sp'))
- output 2: bfloat16 [8192, 256], P(('ens', 'sp'))
All inputs are finite; a program needn't handle non-finite values.
Results may differ from the reference program's by a relative error of at most 0.0159135.
Values are sent between devices in bfloat16 or wider.
A program may use at most 1 GiB of HBM per device.

```python
import jax
import jax.numpy as jnp
from jax import lax

SEQ_LEN = 8192
RES_CH = 256
GATE_CH = 256
SKIP_CH = 256
CLASSES = 256
DIL_CYCLE = 10
STACKS = 2
LAYERS_ALL = STACKS * DIL_CYCLE


def setup_inputs(seed: int = 0, part: int = 0) -> dict:
    root_key = jax.random.key(seed)
    subkeys = jax.random.split(root_key, 10)
    seq_key = jax.random.fold_in(subkeys[0], part)
    conv_shape = (STACKS, DIL_CYCLE, RES_CH, 2 * GATE_CH)
    conv_scale = (2 * RES_CH) ** -0.5
    proj_scale = 2.0 * (GATE_CH * LAYERS_ALL) ** -0.5
    head_scale = 2.0 * SKIP_CH ** -0.5
    x_seq = jax.random.normal(seq_key, (SEQ_LEN, RES_CH), jnp.float32)
    w_past = jax.random.normal(subkeys[1], conv_shape, jnp.float32) * conv_scale
    w_now = jax.random.normal(subkeys[2], conv_shape, jnp.float32) * conv_scale
    b_conv = jax.random.normal(subkeys[3], (STACKS, DIL_CYCLE, 2 * GATE_CH), jnp.float32) * 0.5
    w_res = jax.random.normal(subkeys[4], (STACKS, DIL_CYCLE, GATE_CH, RES_CH), jnp.float32) * proj_scale
    w_skip = jax.random.normal(subkeys[5], (STACKS, DIL_CYCLE, GATE_CH, SKIP_CH), jnp.float32) * proj_scale
    w_out1 = jax.random.normal(subkeys[6], (SKIP_CH, SKIP_CH), jnp.float32) * head_scale
    b_out1 = jax.random.normal(subkeys[7], (SKIP_CH,), jnp.float32) * 0.5
    w_out2 = jax.random.normal(subkeys[8], (SKIP_CH, CLASSES), jnp.float32) * head_scale
    b_out2 = jax.random.normal(subkeys[9], (CLASSES,), jnp.float32) * 0.5
    return {
        "x_seq": x_seq.astype(jnp.bfloat16),
        "w_past": w_past.astype(jnp.bfloat16),
        "w_now": w_now.astype(jnp.bfloat16),
        "b_conv": b_conv,
        "w_res": w_res.astype(jnp.bfloat16),
        "w_skip": w_skip.astype(jnp.bfloat16),
        "w_out1": w_out1.astype(jnp.bfloat16),
        "b_out1": b_out1,
        "w_out2": w_out2.astype(jnp.bfloat16),
        "b_out2": b_out2,
    }


def reference(x_seq, w_past, w_now, b_conv, w_res, w_skip, w_out1, b_out1, w_out2, b_out2):
    def stack_body(carry, stack_w):
        hidden, skip_sum = carry
        past_w, now_w, conv_b, res_w, skip_w = stack_w
        for layer_pos in range(DIL_CYCLE):
            dilation = 2 ** layer_pos
            shifted = jnp.concatenate([jnp.zeros((dilation, RES_CH), hidden.dtype), hidden[:SEQ_LEN - dilation]], axis=0)
            pre_act = (jnp.dot(shifted, past_w[layer_pos], preferred_element_type=jnp.float32)
                       + jnp.dot(hidden, now_w[layer_pos], preferred_element_type=jnp.float32)
                       + conv_b[layer_pos])
            gated = (jnp.tanh(pre_act[:, :GATE_CH]) * jax.nn.sigmoid(pre_act[:, GATE_CH:])).astype(jnp.bfloat16)
            hidden = (hidden.astype(jnp.float32) + jnp.dot(gated, res_w[layer_pos], preferred_element_type=jnp.float32)).astype(jnp.bfloat16)
            skip_sum = skip_sum + jnp.dot(gated, skip_w[layer_pos], preferred_element_type=jnp.float32)
        return (hidden, skip_sum), None

    skip_init = jnp.zeros((SEQ_LEN, SKIP_CH), jnp.float32)
    (hidden, skip_sum), _ = lax.scan(stack_body, (x_seq, skip_init), (w_past, w_now, b_conv, w_res, w_skip))
    skip_act = jax.nn.relu(skip_sum).astype(jnp.bfloat16)
    mid_act = jax.nn.relu(jnp.dot(skip_act, w_out1, preferred_element_type=jnp.float32) + b_out1).astype(jnp.bfloat16)
    logits = jnp.dot(mid_act, w_out2, preferred_element_type=jnp.float32) + b_out2
    return (logits, hidden)
```

```python
import dataclasses

import jax
import jax.numpy as jnp
from jax import lax
from jax.experimental import pallas as pl
from jax.experimental.pallas import tpu as pltpu
from jax.sharding import PartitionSpec as P

F32, BF16 = jnp.float32, jnp.bfloat16
ROWS, CH, LAYERS, CYCLE = 1024, 256, 20, 10
HALO = 512
PIECE = 64
XROWS = 128
EDGE = 128

LAT_Z, LAT_LINK, CYC_ROW = 750, 5200, 10.5


def dil(layer):
    return 2 ** (layer % CYCLE)


@dataclasses.dataclass
class Job:
    layer: int
    start: int
    rows: int
    valid: int
    needs: list = dataclasses.field(default_factory=list)
    halos: list = dataclasses.field(default_factory=list)
    path: float = 0.0

    @property
    def end(self):
        return self.start + self.rows

    @property
    def cost(self):
        return max(1.5 * self.rows * 1.15, 200)


@dataclasses.dataclass
class Head:
    start: int
    rows: int
    needs: list
    path: float = 0.0
    cost: float = 300.0


@dataclasses.dataclass
class Halo:
    layer: int
    start: int
    rows: int
    index: int = 0
    needs: list = dataclasses.field(default_factory=list)
    path: float = 0.0


def plan():
    jobs, halos = [], []

    def add(layer, start, rows, valid=None):
        jobs.append(Job(layer, start, rows, start if valid is None else valid))

    for layer in range(7):
        reach = 2 * dil(layer)
        for start in (768, 512, 256):
            add(layer, start, 256)
        if layer < 6:
            add(layer, 0, 256, reach - 1)
        else:
            add(layer, 64, 192, reach - 1)
        low, high = (-128, 64) if layer < 5 else (-64, 64) if layer == 5 else (0, 128)
        add(layer, low, high - low, reach - EDGE)
    for layer in (7, 8, 9, 17, 18):
        for start in (768, 512, 256, 0):
            add(layer, start, 256)
    for layer in range(10, 17):
        reach = 2 * dil(layer)
        add(layer, 768, 256)
        if layer < 16:
            add(layer, 512, 256, 512 + reach - 1)
            add(layer, 384, 192)
            add(layer, 256, 128, 256 + reach - 1)
            add(layer, 128, 192)
            low = -128 if layer < 15 else -64
            add(layer, low, 128 - low, reach - EDGE)
        else:
            add(layer, 576, 192, 512 + reach - 1)
            add(layer, 448, 192)
            add(layer, 320, 128, 256 + reach - 1)
            add(layer, 192, 192)
            add(layer, 0, 192)
    for start, rows in ((768, 256), (512, 256), (256, 256), (128, 128), (0, 128)):
        add(19, start, rows)

    for layer, rows, chunk in ((0, 128, 128), (7, 128, 128), (8, 256, 256), (9, 512, 256),
                               (10, 128, 128), (17, 128, 128), (18, 256, 256), (19, 512, 128)):
        for top in range(0, rows, chunk):
            halos.append(Halo(layer, -top - chunk, chunk, len(halos)))

    def cover(layer, low, high):
        if layer == 0 or high <= low:
            return []
        found, want = [], set(range(low, high))
        for j in [j for j in jobs if j.layer == layer - 1]:
            have = want & set(range(max(j.valid, j.start), j.end))
            if have:
                found.append(j)
                want -= have
        assert not want, (layer, low, high, sorted(want)[:3])
        return found

    for j in jobs:
        d = dil(j.layer)
        for low, high in ((j.valid, j.end), (j.valid - d, j.end - d)):
            inner = max(low, 0)
            if low < 0 and dil(j.layer) > 64 or low < 0 and j.layer % CYCLE == 0:
                j.halos += [h for h in halos if h.layer == j.layer and h.start < high and h.start + h.rows > low and h not in j.halos]
            elif low < 0:
                inner = low
            j.needs += [k for k in cover(j.layer, inner, high) if k not in j.needs]
    for j in jobs:
        j.needs += [k for k in jobs if k.layer == j.layer and k is not j and k.start < j.end and k.valid > j.start and k.valid > k.start
                    and k not in j.needs and (k.start, k.rows) != (j.start, j.rows) and j.valid < k.valid]
    for h in halos:
        h.needs = cover(h.layer, ROWS + h.start, ROWS + h.start + h.rows)

    heads = [Head(j.start, j.rows, [j] + [k for k in jobs if k.end > j.start and k.start < j.end and k.end > 0])
             for j in jobs if j.layer == LAYERS - 1]

    for head in heads:
        head.path = head.cost + LAT_Z
    for layer in range(LAYERS, -1, -1):
        for j in [j for j in jobs if j.layer == layer]:
            users = [k for k in jobs if k.layer == layer + 1 and j in k.needs]
            sent = [h for h in halos if j in h.needs]
            j.path = j.cost + LAT_Z + max([k.path for k in users] + [h.path for h in sent] + [600])
        for h in [h for h in halos if h.layer == layer]:
            h.path = LAT_LINK + CYC_ROW * h.rows + max(k.path for k in jobs if h in k.halos)

    now, order, done, arrive, link = 0.0, [], {}, {}, 0.0
    left = list(jobs) + heads
    while left:
        for h in halos:
            if h.index not in arrive and all(id(k) in done for k in h.needs):
                begin = max([link] + [done[id(k)] for k in h.needs])
                link = begin + CYC_ROW * h.rows
                arrive[h.index] = link + LAT_LINK
        best = None
        for i in left:
            if not all(id(k) in done for k in i.needs):
                continue
            hs = getattr(i, "halos", [])
            if not all(h.index in arrive for h in hs):
                continue
            ready = max([now] + [done[id(k)] for k in i.needs] + [arrive[h.index] for h in hs])
            key = (max(ready - now, 0), -i.path, -i.start)
            if best is None or key < best[0]:
                best = (key, i, ready)
        _, i, ready = best
        now = max(now, ready) + i.cost
        done[id(i)] = now + LAT_Z
        order.append(i)
        left = [k for k in left if k is not i]
    return order, halos, now


WEIGHT_WAITS = (0, 1, 2, 3, 5, 8, 13, 20)


def dot(a, b):
    return jnp.dot(a, b, preferred_element_type=F32)


def kernel(order, halos, devices, x, wp, wn, b, wr, ws, w1, b1, w2, b2, y, h_out,
           H, S, XH, W, WRS, W1, W2, B, B1, B2, wsem, osem, send_sem, recv_sem):
    me = lax.axis_index("sp")
    first = me == 0

    load_x = pltpu.make_async_copy(x, H.at[0, HALO:HALO + ROWS], wsem.at[LAYERS + 1])
    small = [pltpu.make_async_copy(src, dst, wsem.at[LAYERS + 2 + i])
             for i, (src, dst) in enumerate(((b, B), (b1, B1), (b2, B2)))]
    layer_loads = []
    for layer in range(LAYERS):
        layer_loads.append([pltpu.make_async_copy(wp.at[layer], W.at[layer, 0:CH], wsem.at[layer]),
                            pltpu.make_async_copy(wn.at[layer], W.at[layer, CH:2 * CH], wsem.at[layer]),
                            pltpu.make_async_copy(wr.at[layer], WRS.at[layer, :, 0:CH], wsem.at[layer]),
                            pltpu.make_async_copy(ws.at[layer], WRS.at[layer, :, CH:2 * CH], wsem.at[layer])])
    head_loads = [pltpu.make_async_copy(w1, W1, wsem.at[LAYERS]), pltpu.make_async_copy(w2, W2, wsem.at[LAYERS + 5])]
    for c in [load_x] + layer_loads[0] + small:
        c.start()
    for group in layer_loads[1:]:
        for c in group:
            c.start()
    for c in head_loads:
        c.start()

    @pl.when(first)
    def _():
        XH[...] = jnp.zeros_like(XH)
        for h in halos:
            if h.layer:
                H[h.layer, HALO + h.start:HALO + h.start + h.rows] = jnp.zeros((h.rows, CH), BF16)

    barrier = pltpu.get_barrier_semaphore()

    @pl.when(me > 0)
    def _():
        pl.semaphore_signal(barrier, inc=1, device_id={"sp": me - 1}, device_id_type=pl.DeviceIdType.MESH)

    @pl.when(me < devices - 1)
    def _():
        pl.semaphore_wait(barrier, 1)

    def remote(h):
        src = H.at[h.layer, HALO + ROWS + h.start:HALO + ROWS + h.start + h.rows]
        dst = H.at[h.layer, HALO + h.start:HALO + h.start + h.rows] if h.layer else XH.at[XROWS + h.start:XROWS + h.start + h.rows]
        return pltpu.make_async_remote_copy(
            src_ref=src, dst_ref=dst, send_sem=send_sem.at[h.index], recv_sem=recv_sem.at[h.index],
            device_id={"sp": lax.rem(me + 1, devices)}, device_id_type=pl.DeviceIdType.MESH)

    finished, sent, arrived, weighed, added, reads = set(), set(), set(), set(), set(), []

    def wait_for(item):
        if isinstance(item, Job):
            if item.layer not in weighed:
                low = max(k for k in WEIGHT_WAITS if k <= item.layer)
                high = min(k for k in WEIGHT_WAITS if k > item.layer)
                for layer in range(low, high):
                    weighed.add(layer)
                    for c in layer_loads[layer]:
                        c.wait()
            for h in item.halos:
                if h.index not in arrived:
                    arrived.add(h.index)
                    pl.when(me > 0)(remote(h).wait_recv)
                    if not h.layer:
                        H[0, HALO + h.start:HALO + h.start + h.rows] = XH[XROWS + h.start:XROWS + h.start + h.rows]
        elif isinstance(item, Head) and "head" not in weighed:
            weighed.add("head")
            for c in head_loads:
                c.wait()

    def send_ready():
        for h in halos:
            if h.index not in sent and all(id(k) in finished for k in h.needs):
                sent.add(h.index)
                pl.when(me < devices - 1)(remote(h).start)

    def write_back(src, dst, index):
        c = pltpu.make_async_copy(src, dst, osem.at[index])
        c.start()
        reads.append(c)

    def z_stage(item):
        at, d = HALO + item.start, dil(item.layer)
        both = jnp.concatenate([H[item.layer, at - d:at - d + item.rows], H[item.layer, at:at + item.rows]], axis=1)
        return dot(both, W[item.layer])

    def gate_stage(item, z):
        z = z + B[item.layer // CYCLE, item.layer % CYCLE:item.layer % CYCLE + 1]
        t = jnp.tanh(z[:, :CH])
        u = jnp.tanh(0.5 * z[:, CH:])
        return (0.5 * (t * u + t)).astype(BF16)

    def fin_stage(item, g):
        at = HALO + item.start
        rs = dot(g, WRS[item.layer])
        new = (H[item.layer, at:at + item.rows].astype(F32) + rs[:, :CH]).astype(BF16)
        if item.start < 0:
            cut = min(-item.start, item.rows)
            top = jnp.where(first, jnp.zeros((cut, CH), BF16), new[:cut])
            H[item.layer + 1, at:at + cut] = top
            if cut < item.rows:
                H[item.layer + 1, at + cut:at + item.rows] = new[cut:]
        else:
            H[item.layer + 1, at:at + item.rows] = new
        fresh = [i for i in range(0, item.rows, PIECE)
                 if item.start + i >= max(item.valid, 0) and (item.layer, item.start + i) not in added]
        added.update((item.layer, item.start + i) for i in fresh)
        if fresh:
            low, high = fresh[0], fresh[-1] + PIECE
            assert high - low == len(fresh) * PIECE
            rows = slice(item.start + low, item.start + high)
            part = rs[low:high, CH:]
            S[rows] = part if item.layer == 0 else S[rows] + part
        finished.add(id(item))

    pipe = []

    def retire(upto):
        while len(pipe) > upto:
            item, z = pipe.pop(0)
            fin_stage(item, gate_stage(item, z))
            if item.layer == LAYERS - 1:
                write_back(H.at[LAYERS, HALO + item.start:HALO + item.end], h_out.at[item.start:item.end], len(reads))
            send_ready()

    def head_stage(item):
        rows = slice(item.start, item.start + item.rows)
        a = jnp.maximum(S[rows], 0.0).astype(BF16)
        m = jnp.maximum(dot(a, W1[...]) + B1[...], 0.0).astype(BF16)
        S[rows] = dot(m, W2[...]) + B2[...]
        write_back(S.at[item.start:item.start + item.rows], y.at[item.start:item.start + item.rows], len(reads))

    load_x.wait()
    send_ready()
    for c in small:
        c.wait()
    for item in order:
        while pipe and not all(id(k) in finished for k in item.needs):
            retire(len(pipe) - 1)
        assert all(id(k) in finished for k in item.needs)
        wait_for(item)
        if isinstance(item, Head):
            head_stage(item)
            continue
        pipe.append((item, z_stage(item)))
        retire(1)
    retire(0)
    for c in reads:
        c.wait()

    @pl.when(me < devices - 1)
    def _():
        for h in halos:
            remote(h).wait_send()


def solution(mesh):
    devices = mesh.shape["sp"]
    order, halos, _ = plan()
    rows = P(("ens", "sp"), None)
    outs = sum(isinstance(i, Head) for i in order) + sum(isinstance(i, Job) and i.layer == LAYERS - 1 for i in order)

    def local(x, wp, wn, b, wr, ws, w1, b1, w2, b2):
        hbm = pl.BlockSpec(memory_space=pltpu.HBM)
        vmem = lambda *shape: pltpu.VMEM(shape, BF16)
        return pl.pallas_call(
            lambda *refs: kernel(order, halos, devices, *refs),
            out_shape=(jax.ShapeDtypeStruct((ROWS, CH), F32), jax.ShapeDtypeStruct((ROWS, CH), BF16)),
            in_specs=[hbm] * 10,
            out_specs=(hbm, hbm),
            scratch_shapes=[
                vmem(LAYERS + 1, HALO + ROWS, CH), pltpu.VMEM((ROWS, CH), F32), vmem(XROWS, CH),
                vmem(LAYERS, 2 * CH, 2 * CH), vmem(LAYERS, CH, 2 * CH), vmem(CH, CH), vmem(CH, CH),
                pltpu.VMEM((LAYERS // CYCLE, CYCLE, 2 * CH), F32), pltpu.VMEM((1, CH), F32), pltpu.VMEM((1, CH), F32),
                pltpu.SemaphoreType.DMA((LAYERS + 6,)), pltpu.SemaphoreType.DMA((outs,)),
                pltpu.SemaphoreType.DMA((len(halos),)), pltpu.SemaphoreType.DMA((len(halos),)),
            ],
            compiler_params=pltpu.CompilerParams(collective_id=0, has_side_effects=True, vmem_limit_bytes=62 * 1024 * 1024),
            name="wavenet_stack",
        )(x, wp.reshape(LAYERS, CH, 2 * CH), wn.reshape(LAYERS, CH, 2 * CH), b,
          wr.reshape(LAYERS, CH, CH), ws.reshape(LAYERS, CH, CH), w1, b1.reshape(1, CH), w2, b2.reshape(1, CH))

    return jax.shard_map(local, mesh=mesh, in_specs=(rows,) + (P(),) * 9, out_specs=(rows, rows), check_vma=False)
```

```python
import dataclasses

import jax
import jax.numpy as jnp
from jax import lax
from jax.experimental import pallas as pl
from jax.experimental.pallas import tpu as pltpu
from jax.sharding import PartitionSpec as P

F32, BF16 = jnp.float32, jnp.bfloat16
ROWS, CH, LAYERS, CYCLE = 1024, 256, 20, 10
HALO = 512
PIECE = 64
XROWS = 128
EDGE = 128

LAT_Z, LAT_LINK, CYC_ROW = 750, 5200, 10.5


def dil(layer):
    return 2 ** (layer % CYCLE)


@dataclasses.dataclass
class Job:
    layer: int
    start: int
    rows: int
    valid: int
    needs: list = dataclasses.field(default_factory=list)
    halos: list = dataclasses.field(default_factory=list)
    path: float = 0.0

    @property
    def end(self):
        return self.start + self.rows

    @property
    def cost(self):
        return max(1.5 * self.rows * 1.15, 200)


@dataclasses.dataclass
class Halo:
    layer: int
    start: int
    rows: int
    index: int = 0
    needs: list = dataclasses.field(default_factory=list)
    path: float = 0.0


def plan():
    jobs, halos = [], []

    def add(layer, start, rows, valid=None):
        jobs.append(Job(layer, start, rows, start if valid is None else valid))

    for layer in range(7):
        reach = 2 * dil(layer)
        for start in (768, 512, 256):
            add(layer, start, 256)
        if layer < 6:
            add(layer, 0, 256, reach - 1)
        else:
            add(layer, 64, 192, reach - 1)
        low, high = (-128, 64) if layer < 5 else (-64, 64) if layer == 5 else (0, 128)
        add(layer, low, high - low, reach - EDGE)
    for layer in (7, 8, 9, 17, 18):
        for start in (768, 512, 256, 0):
            add(layer, start, 256)
    for layer in range(10, 17):
        reach = 2 * dil(layer)
        add(layer, 768, 256)
        if layer < 16:
            add(layer, 512, 256, 512 + reach - 1)
            add(layer, 384, 192)
            add(layer, 256, 128, 256 + reach - 1)
            add(layer, 128, 192)
            low = -128 if layer < 15 else -64
            add(layer, low, 128 - low, reach - EDGE)
        else:
            add(layer, 576, 192, 512 + reach - 1)
            add(layer, 448, 192)
            add(layer, 320, 128, 256 + reach - 1)
            add(layer, 192, 192)
            add(layer, 0, 192)
    for start, rows in ((768, 256), (512, 256), (256, 256), (128, 128), (0, 128)):
        add(19, start, rows)

    for layer, rows, chunk in ((0, 128, 128), (7, 128, 128), (8, 256, 256), (9, 512, 256),
                               (10, 128, 128), (17, 128, 128), (18, 256, 256), (19, 512, 128)):
        for top in range(0, rows, chunk):
            halos.append(Halo(layer, -top - chunk, chunk, len(halos)))

    def cover(layer, low, high):
        if layer == 0 or high <= low:
            return []
        found, want = [], set(range(low, high))
        for j in [j for j in jobs if j.layer == layer - 1]:
            have = want & set(range(max(j.valid, j.start), j.end))
            if have:
                found.append(j)
                want -= have
        assert not want, (layer, low, high, sorted(want)[:3])
        return found

    for j in jobs:
        d = dil(j.layer)
        for low, high in ((j.valid, j.end), (j.valid - d, j.end - d)):
            inner = max(low, 0)
            if low < 0 and dil(j.layer) > 64 or low < 0 and j.layer % CYCLE == 0:
                j.halos += [h for h in halos if h.layer == j.layer and h.start < high and h.start + h.rows > low and h not in j.halos]
            elif low < 0:
                inner = low
            j.needs += [k for k in cover(j.layer, inner, high) if k not in j.needs]
    for j in jobs:
        j.needs += [k for k in jobs if k.layer == j.layer and k is not j and k.start < j.end and k.valid > j.start and k.valid > k.start
                    and k not in j.needs and (k.start, k.rows) != (j.start, j.rows) and j.valid < k.valid]
    for h in halos:
        h.needs = cover(h.layer, ROWS + h.start, ROWS + h.start + h.rows)

    for layer in range(LAYERS, -1, -1):
        for j in [j for j in jobs if j.layer == layer]:
            users = [k for k in jobs if k.layer == layer + 1 and j in k.needs]
            sent = [h for h in halos if j in h.needs]
            j.path = j.cost + LAT_Z + max([k.path for k in users] + [h.path for h in sent] + [600])
        for h in [h for h in halos if h.layer == layer]:
            h.path = LAT_LINK + CYC_ROW * h.rows + max(k.path for k in jobs if h in k.halos)

    now, order, done, arrive, link = 0.0, [], {}, {}, 0.0
    left = list(jobs)
    while left:
        for h in halos:
            if h.index not in arrive and all(id(k) in done for k in h.needs):
                begin = max([link] + [done[id(k)] for k in h.needs])
                link = begin + CYC_ROW * h.rows
                arrive[h.index] = link + LAT_LINK
        best = None
        for i in left:
            if not all(id(k) in done for k in i.needs):
                continue
            hs = getattr(i, "halos", [])
            if not all(h.index in arrive for h in hs):
                continue
            ready = max([now] + [done[id(k)] for k in i.needs] + [arrive[h.index] for h in hs])
            key = (max(ready - now, 0), -i.path, -i.start)
            if best is None or key < best[0]:
                best = (key, i, ready)
        _, i, ready = best
        now = max(now, ready) + i.cost
        done[id(i)] = now + LAT_Z
        order.append(i)
        left = [k for k in left if k is not i]
    return order, halos, now


HEAD_ROWS = 256
WEIGHT_WAITS = (0, 1, 2, 3, 5, 8, 13, 20)


def dot(a, b):
    return jnp.dot(a, b, preferred_element_type=F32)


def stack_kernel(order, halos, devices, x, wp, wn, b, wr, ws, S, h_out,
                 H, XH, W, WRS, B, wsem, send_sem, recv_sem):
    me = lax.axis_index("sp")
    first = me == 0

    load_x = pltpu.make_async_copy(x, H.at[0, HALO:HALO + ROWS], wsem.at[LAYERS + 1])
    load_b = pltpu.make_async_copy(b, B, wsem.at[LAYERS])
    layer_loads = []
    for layer in range(LAYERS):
        layer_loads.append([pltpu.make_async_copy(wp.at[layer], W.at[layer, 0:CH], wsem.at[layer]),
                            pltpu.make_async_copy(wn.at[layer], W.at[layer, CH:2 * CH], wsem.at[layer]),
                            pltpu.make_async_copy(wr.at[layer], WRS.at[layer, :, 0:CH], wsem.at[layer]),
                            pltpu.make_async_copy(ws.at[layer], WRS.at[layer, :, CH:2 * CH], wsem.at[layer])])
    for c in [load_x] + layer_loads[0] + [load_b]:
        c.start()
    for group in layer_loads[1:]:
        for c in group:
            c.start()

    @pl.when(first)
    def _():
        XH[...] = jnp.zeros_like(XH)
        for h in halos:
            if h.layer:
                H[h.layer, HALO + h.start:HALO + h.start + h.rows] = jnp.zeros((h.rows, CH), BF16)

    barrier = pltpu.get_barrier_semaphore()

    @pl.when(me > 0)
    def _():
        pl.semaphore_signal(barrier, inc=1, device_id={"sp": me - 1}, device_id_type=pl.DeviceIdType.MESH)

    @pl.when(me < devices - 1)
    def _():
        pl.semaphore_wait(barrier, 1)

    def remote(h):
        src = H.at[h.layer, HALO + ROWS + h.start:HALO + ROWS + h.start + h.rows]
        dst = H.at[h.layer, HALO + h.start:HALO + h.start + h.rows] if h.layer else XH.at[XROWS + h.start:XROWS + h.start + h.rows]
        return pltpu.make_async_remote_copy(
            src_ref=src, dst_ref=dst, send_sem=send_sem.at[h.index], recv_sem=recv_sem.at[h.index],
            device_id={"sp": lax.rem(me + 1, devices)}, device_id_type=pl.DeviceIdType.MESH)

    finished, sent, arrived, weighed, added = set(), set(), set(), set(), set()

    def wait_for(item):
        if item is not None:
            if item.layer not in weighed:
                low = max(k for k in WEIGHT_WAITS if k <= item.layer)
                high = min(k for k in WEIGHT_WAITS if k > item.layer)
                for layer in range(low, high):
                    weighed.add(layer)
                    for c in layer_loads[layer]:
                        c.wait()
            for h in item.halos:
                if h.index not in arrived:
                    arrived.add(h.index)
                    pl.when(me > 0)(remote(h).wait_recv)
                    if not h.layer:
                        H[0, HALO + h.start:HALO + h.start + h.rows] = XH[XROWS + h.start:XROWS + h.start + h.rows]

    def send_ready():
        for h in halos:
            if h.index not in sent and all(id(k) in finished for k in h.needs):
                sent.add(h.index)
                pl.when(me < devices - 1)(remote(h).start)

    def z_stage(item):
        at, d = HALO + item.start, dil(item.layer)
        both = jnp.concatenate([H[item.layer, at - d:at - d + item.rows], H[item.layer, at:at + item.rows]], axis=1)
        return dot(both, W[item.layer])

    def gate_stage(item, z):
        z = z + B[item.layer // CYCLE, item.layer % CYCLE:item.layer % CYCLE + 1]
        t = jnp.tanh(z[:, :CH])
        u = jnp.tanh(0.5 * z[:, CH:])
        return (0.5 * (t * u + t)).astype(BF16)

    def fin_stage(item, rs):
        at = HALO + item.start
        new = (H[item.layer, at:at + item.rows].astype(F32) + rs[:, :CH]).astype(BF16)
        if item.start < 0:
            cut = min(-item.start, item.rows)
            top = jnp.where(first, jnp.zeros((cut, CH), BF16), new[:cut])
            H[item.layer + 1, at:at + cut] = top
            if cut < item.rows:
                H[item.layer + 1, at + cut:at + item.rows] = new[cut:]
        elif item.layer < LAYERS - 1:
            H[item.layer + 1, at:at + item.rows] = new
        else:
            h_out[item.start:item.end] = new
        fresh = [i for i in range(0, item.rows, PIECE)
                 if item.start + i >= max(item.valid, 0) and (item.layer, item.start + i) not in added]
        added.update((item.layer, item.start + i) for i in fresh)
        if fresh:
            low, high = fresh[0], fresh[-1] + PIECE
            assert high - low == len(fresh) * PIECE
            rows = slice(item.start + low, item.start + high)
            part = rs[low:high, CH:]
            S[rows] = part if item.layer == 0 else S[rows] + part
        finished.add(id(item))

    pipe = []

    def step(item, coming):
        g = gate_stage(item, z_stage(item)) if item is not None else None
        send_ready()
        wait_for(coming)
        if pipe:
            done, gated = pipe.pop()
            fin_stage(done, dot(gated, WRS[done.layer]))
        if item is not None:
            pipe.append((item, g))

    load_x.wait()
    send_ready()
    load_b.wait()
    wait_for(order[0])
    for n, item in enumerate(order):
        while not all(id(k) in finished for k in item.needs):
            assert pipe
            step(None, item)
        coming = order[n + 1] if n + 1 < len(order) else None
        step(item, coming)
    while pipe:
        step(None, None)

    @pl.when(me < devices - 1)
    def _():
        for h in halos:
            remote(h).wait_send()


def head_kernel(S, h, w1, b1, w2, b2, y, h_out, Y, sem):
    pass_h = pltpu.make_async_copy(h, h_out, sem.at[0])
    pass_h.start()
    writes = []
    for n, start in enumerate(range(0, ROWS, HEAD_ROWS)):
        rows = slice(start, start + HEAD_ROWS)
        a = jnp.maximum(S[rows], 0.0).astype(BF16)
        m = jnp.maximum(dot(a, w1[...]) + b1[...], 0.0).astype(BF16)
        Y[rows] = dot(m, w2[...]) + b2[...]
        c = pltpu.make_async_copy(Y.at[rows], y.at[rows], sem.at[1 + n])
        c.start()
        writes.append(c)
    pass_h.wait()
    for c in writes:
        c.wait()


def solution(mesh):
    devices = mesh.shape["sp"]
    order, halos, _ = plan()
    rows = P(("ens", "sp"), None)

    def local(x, wp, wn, b, wr, ws, w1, b1, w2, b2):
        hbm, near = pl.BlockSpec(memory_space=pltpu.HBM), pl.BlockSpec(memory_space=pltpu.VMEM)
        vmem = lambda *shape: pltpu.VMEM(shape, BF16)
        skip, hidden = pl.pallas_call(
            lambda *refs: stack_kernel(order, halos, devices, *refs),
            out_shape=(pltpu.VMEM((ROWS, CH), F32), pltpu.VMEM((ROWS, CH), BF16)),
            in_specs=[hbm] * 6,
            out_specs=(near, near),
            scratch_shapes=[
                vmem(LAYERS, HALO + ROWS, CH), vmem(XROWS, CH),
                vmem(LAYERS, 2 * CH, 2 * CH), vmem(LAYERS, CH, 2 * CH),
                pltpu.VMEM((LAYERS // CYCLE, CYCLE, 2 * CH), F32),
                pltpu.SemaphoreType.DMA((LAYERS + 2,)),
                pltpu.SemaphoreType.DMA((len(halos),)), pltpu.SemaphoreType.DMA((len(halos),)),
            ],
            compiler_params=pltpu.CompilerParams(collective_id=0, has_side_effects=True, vmem_limit_bytes=56 * 1024 * 1024),
            name="wavenet_stack",
        )(x, wp.reshape(LAYERS, CH, 2 * CH), wn.reshape(LAYERS, CH, 2 * CH), b,
          wr.reshape(LAYERS, CH, CH), ws.reshape(LAYERS, CH, CH))
        return pl.pallas_call(
            head_kernel,
            out_shape=(jax.ShapeDtypeStruct((ROWS, CH), F32), jax.ShapeDtypeStruct((ROWS, CH), BF16)),
            in_specs=[near] * 6,
            out_specs=(hbm, hbm),
            scratch_shapes=[pltpu.VMEM((ROWS, CH), F32), pltpu.SemaphoreType.DMA((1 + ROWS // HEAD_ROWS,))],
            compiler_params=pltpu.CompilerParams(vmem_limit_bytes=6 * 1024 * 1024),
            name="wavenet_head",
        )(skip, hidden, w1, b1.reshape(1, CH), w2, b2.reshape(1, CH))

    return jax.shard_map(local, mesh=mesh, in_specs=(rows,) + (P(),) * 9, out_specs=(rows, rows), check_vma=False)
```

```python
import dataclasses

import jax
import jax.numpy as jnp
from jax import lax
from jax.experimental import pallas as pl
from jax.experimental.pallas import tpu as pltpu
from jax.sharding import PartitionSpec as P

F32, BF16 = jnp.float32, jnp.bfloat16
ROWS, CH, LAYERS, CYCLE = 1024, 256, 20, 10
HALO = 512
XROWS = 128
TILE = 256


def dil(layer):
    return 2 ** (layer % CYCLE)


@dataclasses.dataclass(frozen=True)
class Job:
    layer: int
    start: int
    rows: int
    needs: tuple
    halos: tuple

    @property
    def end(self):
        return self.start + self.rows


@dataclasses.dataclass(frozen=True)
class Halo:
    layer: int
    start: int
    rows: int
    index: int
    needs: tuple


JOBS = (
    (0, 768, 256, (), ()), (0, 512, 256, (), ()), (0, 256, 256, (), ()),
    (0, 0, 256, (), ()), (0, -128, 192, (3,), (0,)), (1, 768, 256, (0, 1), ()),
    (1, 512, 256, (1, 2), ()), (1, 256, 256, (2, 3), ()), (1, 0, 256, (3,), ()),
    (1, -128, 192, (3, 4, 8), ()), (2, 768, 256, (5, 6), ()), (2, 512, 256, (6, 7), ()),
    (2, 256, 256, (7, 8), ()), (2, 0, 256, (8,), ()), (2, -128, 192, (8, 9, 13), ()),
    (3, 768, 256, (10, 11), ()), (3, 512, 256, (11, 12), ()), (3, 256, 256, (12, 13), ()),
    (3, 0, 256, (13,), ()), (3, -128, 192, (13, 14, 18), ()), (4, 768, 256, (15, 16), ()),
    (4, 512, 256, (16, 17), ()), (4, 256, 256, (17, 18), ()), (4, 0, 256, (18,), ()),
    (4, -128, 192, (18, 19, 23), ()), (5, 768, 256, (20, 21), ()), (5, 512, 256, (21, 22), ()),
    (5, 256, 256, (22, 23), ()), (5, 0, 256, (23,), ()), (5, -64, 128, (23, 24, 28), ()),
    (6, 768, 256, (25, 26), ()), (6, 512, 256, (26, 27), ()), (6, 256, 256, (27, 28), ()),
    (6, 64, 192, (28,), ()), (6, 0, 128, (28, 29, 33), ()), (7, 768, 256, (30, 31), ()),
    (7, 512, 256, (31, 32), ()), (7, 256, 256, (32, 33), ()), (7, 0, 256, (33, 34), (1,)),
    (8, 768, 256, (35, 36), ()), (8, 512, 256, (36, 37), ()), (8, 256, 256, (37, 38), ()),
    (8, 0, 256, (38,), (2,)), (9, 768, 256, (39, 41), ()), (9, 512, 256, (40, 42), ()),
    (9, 256, 256, (41,), (3,)), (9, 0, 256, (42,), (4,)), (17, 768, 256, (91, 92), ()),
    (17, 512, 256, (92, 93, 94), ()), (17, 256, 256, (93, 94, 95, 96), ()), (17, 0, 256, (95, 96), (6,)),
    (18, 768, 256, (47, 48), ()), (18, 512, 256, (48, 49), ()), (18, 256, 256, (49, 50), ()),
    (18, 0, 256, (50,), (7,)), (10, 768, 256, (43, 44), ()), (10, 512, 256, (44,), ()),
    (10, 384, 192, (44, 45, 56), ()), (10, 256, 128, (45,), ()), (10, 64, 256, (45, 46, 58), ()),
    (10, -128, 192, (46,), (5,)), (11, 768, 256, (55, 56), ()), (11, 512, 256, (56,), ()),
    (11, 384, 192, (56, 57, 58, 62), ()), (11, 256, 128, (58,), ()), (11, 64, 256, (58, 59, 60, 64), ()),
    (11, -128, 192, (60,), ()), (12, 768, 256, (61, 62), ()), (12, 512, 256, (62,), ()),
    (12, 384, 192, (62, 63, 64, 68), ()), (12, 256, 128, (64,), ()), (12, 64, 256, (64, 65, 66, 70), ()),
    (12, -128, 192, (66,), ()), (13, 768, 256, (67, 68), ()), (13, 512, 256, (68,), ()),
    (13, 384, 192, (68, 69, 70, 74), ()), (13, 256, 128, (70,), ()), (13, 64, 256, (70, 71, 72, 76), ()),
    (13, -128, 192, (72,), ()), (14, 768, 256, (73, 74), ()), (14, 512, 256, (74,), ()),
    (14, 384, 192, (74, 75, 76, 80), ()), (14, 256, 128, (76,), ()), (14, 64, 256, (76, 77, 78, 82), ()),
    (14, -128, 192, (78,), ()), (15, 768, 256, (79, 80), ()), (15, 512, 256, (80,), ()),
    (15, 384, 192, (80, 81, 82, 86), ()), (15, 256, 128, (82,), ()), (15, 128, 192, (82, 83, 88), ()),
    (15, -64, 192, (83, 84), ()), (16, 768, 256, (85, 86), ()), (16, 576, 192, (86,), ()),
    (16, 448, 192, (86, 87, 92), ()), (16, 320, 128, (87, 88), ()), (16, 192, 192, (88, 89, 94), ()),
    (16, 0, 192, (89, 90), ()), (19, 768, 256, (51, 53), ()), (19, 512, 256, (52, 54), ()),
    (19, 256, 256, (53,), (8, 9)), (19, 128, 128, (54,), (10,)), (19, 0, 128, (54,), (11,)),
)
HALOS = (
    (0, -128, 128, ()), (7, -128, 128, (30,)), (8, -256, 256, (35,)),
    (9, -256, 256, (39,)), (9, -512, 256, (40,)), (10, -128, 128, (43,)),
    (17, -128, 128, (91,)), (18, -256, 256, (47,)), (19, -128, 128, (51,)),
    (19, -256, 128, (51,)), (19, -384, 128, (52,)), (19, -512, 128, (52,)),
)
STEPS = (
    ("J", 0, ()), ("J", 2, ()), ("J", 3, ()), ("J", 1, ()), ("J", 8, ()), ("J", 7, ()), ("J", 6, ()), ("J", 5, ()),
    ("J", 12, ()), ("J", 11, ()), ("J", 10, ()), ("J", 13, ()), ("J", 16, ()), ("J", 15, ()), ("J", 17, ()), ("J", 18, ()),
    ("J", 20, ()), ("J", 21, ()), ("J", 22, ()), ("J", 23, ()), ("J", 25, ()), ("J", 26, ()), ("J", 27, ()), ("J", 28, ()),
    ("J", 30, ()), ("J", 31, ()), ("J", 32, ()), ("J", 33, (1,)), ("J", 35, ()), ("J", 36, ()), ("J", 37, (2,)), ("J", 4, ()),
    ("J", 39, ()), ("J", 40, ()), ("J", 9, ()), ("S", (0, 2, 512)), ("F", (3,)), ("J", 14, ()), ("S", (2, 2, 512)), ("F", ()),
    ("J", 19, ()), ("S", (4, 2, 512)), ("F", (4,)), ("J", 24, ()), ("S", (6, 2, 512)), ("F", ()), ("J", 29, ()), ("S", (0, 2, 0)),
    ("F", ()), ("J", 34, ()), ("S", (2, 2, 0)), ("F", ()), ("J", 38, ()), ("S", (4, 2, 0)), ("F", ()), ("J", 41, ()),
    ("S", (6, 2, 0)), ("F", ()), ("J", 43, ()), ("J", 42, ()), ("F", ()), ("J", 44, ()), ("F", ()), ("J", 56, ()),
    ("J", 55, ()), ("J", 62, (5,)), ("J", 45, ()), ("J", 61, ()), ("J", 68, ()), ("J", 57, ()), ("J", 67, ()), ("J", 74, ()),
    ("J", 58, ()), ("J", 73, ()), ("J", 80, ()), ("J", 46, ()), ("J", 79, ()), ("J", 86, ()), ("J", 59, ()), ("J", 85, ()),
    ("J", 63, ()), ("J", 64, ()), ("J", 91, ()), ("J", 92, ()), ("J", 69, ()), ("J", 70, (6,)), ("J", 60, ()), ("J", 47, ()),
    ("J", 75, ()), ("J", 76, ()), ("J", 66, ()), ("J", 65, ()), ("J", 81, (7,)), ("J", 82, ()), ("J", 71, ()), ("J", 72, ()),
    ("J", 88, ()), ("J", 87, ()), ("J", 78, ()), ("J", 77, ()), ("J", 94, ()), ("J", 93, ()), ("J", 83, ()), ("J", 84, ()),
    ("J", 48, ()), ("J", 89, ()), ("J", 90, ()), ("J", 51, ()), ("J", 95, ()), ("J", 96, (8,)), ("F", ()), ("J", 49, (9,)),
    ("J", 50, ()), ("J", 52, ()), ("J", 53, ()), ("S", (8, 2, 512)), ("F", (10, 11)), ("J", 54, ()), ("J", 97, ()), ("J", 98, ()),
    ("S", (10, 2, 512)), ("S", (12, 2, 512)), ("S", (14, 2, 512)), ("S", (16, 2, 512)), ("S", (18, 1, 512)), ("S", (8, 2, 0)), ("S", (10, 2, 0)), ("S", (12, 2, 0)),
    ("S", (14, 2, 0)), ("S", (16, 2, 0)), ("S", (18, 1, 0)), ("F", ()), ("J", 99, ()), ("F", ()), ("J", 100, ()), ("F", ()),
    ("J", 101, ()),
)


def plan():
    jobs = [Job(*j) for j in JOBS]
    halos = [Halo(h[0], h[1], h[2], n, h[3]) for n, h in enumerate(HALOS)]
    return jobs, halos, STEPS


HEAD_ROWS = 256
WEIGHT_WAITS = (0, 1, 3, 7, 20)


def dot(a, b):
    return jnp.dot(a, b, preferred_element_type=F32)


def stack_kernel(jobs, halos, steps, devices, x, wp, wn, b, wr, ws, S, h_out,
                 H, XH, G, W, WR, WS, B, wsem, send_sem, recv_sem):
    me = lax.axis_index("sp")
    first = me == 0

    load_x = pltpu.make_async_copy(x, H.at[0, HALO:HALO + ROWS], wsem.at[LAYERS + 1])
    load_b = pltpu.make_async_copy(b, B, wsem.at[LAYERS])
    layer_loads = []
    for layer in range(LAYERS):
        layer_loads.append([pltpu.make_async_copy(wp.at[layer], W.at[layer, 0:CH], wsem.at[layer]),
                            pltpu.make_async_copy(wn.at[layer], W.at[layer, CH:2 * CH], wsem.at[layer]),
                            pltpu.make_async_copy(wr.at[layer], WR.at[layer], wsem.at[layer])])
    load_skip = pltpu.make_async_copy(ws, WS, wsem.at[LAYERS + 2])
    for c in [load_x] + layer_loads[0] + [load_b]:
        c.start()
    for group in layer_loads[1:]:
        for c in group:
            c.start()
    load_skip.start()

    @pl.when(first)
    def _():
        XH[...] = jnp.zeros_like(XH)
        for h in halos:
            if h.layer:
                H[h.layer, HALO + h.start:HALO + h.start + h.rows] = jnp.zeros((h.rows, CH), BF16)

    barrier = pltpu.get_barrier_semaphore()

    @pl.when(me > 0)
    def _():
        pl.semaphore_signal(barrier, inc=1, device_id={"sp": me - 1}, device_id_type=pl.DeviceIdType.MESH)

    @pl.when(me < devices - 1)
    def _():
        pl.semaphore_wait(barrier, 1)

    def remote(h):
        src = H.at[h.layer, HALO + ROWS + h.start:HALO + ROWS + h.start + h.rows]
        dst = H.at[h.layer, HALO + h.start:HALO + h.start + h.rows] if h.layer else XH.at[XROWS + h.start:XROWS + h.start + h.rows]
        return pltpu.make_async_remote_copy(
            src_ref=src, dst_ref=dst, send_sem=send_sem.at[h.index], recv_sem=recv_sem.at[h.index],
            device_id={"sp": lax.rem(me + 1, devices)}, device_id_type=pl.DeviceIdType.MESH)

    finished, gated, arrived, weighed, summed = set(), set(), set(), set(), set()

    def wait_for(n):
        layer, skip_too = jobs[n].layer, "skip" not in weighed
        if layer not in weighed:
            low = max(k for k in WEIGHT_WAITS if k <= layer)
            high = min(k for k in WEIGHT_WAITS if k > layer)
            for k in range(low, high):
                weighed.add(k)
                for c in layer_loads[k]:
                    c.wait()
            if high == LAYERS and skip_too:
                weighed.add("skip")
                load_skip.wait()
        for h in jobs[n].halos:
            if h not in arrived:
                arrived.add(h)
                pl.when(me > 0)(remote(halos[h]).wait_recv)
                if not halos[h].layer:
                    H[0, HALO - XROWS:HALO] = XH[...]

    def send(which):
        for h in which:
            assert finished.issuperset(halos[h].needs)
            pl.when(me < devices - 1)(remote(halos[h]).start)

    def z_stage(job):
        at, d = HALO + job.start, dil(job.layer)
        both = jnp.concatenate([H[job.layer, at - d:at - d + job.rows], H[job.layer, at:at + job.rows]], axis=1)
        return dot(both, W[job.layer])

    def gate_stage(job, z):
        z = z + B[job.layer % CYCLE, job.layer // CYCLE:job.layer // CYCLE + 1]
        t = jnp.tanh(z[:, :CH])
        u = jnp.tanh(0.5 * z[:, CH:])
        g = (0.5 * (t * u + t)).astype(BF16)
        cut = max(-job.start, 0)
        if cut < job.rows and job.layer < LAYERS - 1:
            G[job.start + cut:job.end, job.layer * CH:(job.layer + 1) * CH] = g[cut:]
        return g

    def fin_stage(n, g):
        job = jobs[n]
        at = HALO + job.start
        new = (H[job.layer, at:at + job.rows].astype(F32) + dot(g, WR[job.layer])).astype(BF16)
        if job.layer == LAYERS - 1:
            h_out[job.start:job.end] = new
            add_skip(slice(job.start, job.end), dot(g, WS[(LAYERS - 1) * CH:]))
        elif job.start < 0:
            cut = min(-job.start, job.rows)
            H[job.layer + 1, at:at + cut] = jnp.where(first, jnp.zeros((cut, CH), BF16), new[:cut])
            if cut < job.rows:
                H[job.layer + 1, at + cut:at + job.rows] = new[cut:]
        else:
            H[job.layer + 1, at:at + job.rows] = new
        finished.add(n)

    def add_skip(rows, part):
        S[rows] = S[rows] + part if rows.start // TILE in summed else part

    def skip_stage(layer, count, start):
        for low in (start, start + TILE):
            rows = slice(low, low + TILE)
            add_skip(rows, dot(G[rows, layer * CH:(layer + count) * CH], WS[layer * CH:(layer + count) * CH]))
            summed.add(low // TILE)

    pipe = []

    def retire():
        n, g = pipe.pop()
        fin_stage(n, g)

    load_x.wait()
    send([n for n, h in enumerate(halos) if not h.layer])
    load_b.wait()
    for at, step in enumerate(steps):
        if step[0] == "S":
            assert "skip" in weighed
            skip_stage(*step[1])
            continue
        if step[0] == "J":
            n = step[1]
            assert finished.issuperset(jobs[n].needs), jobs[n]
            wait_for(n)
            g = gate_stage(jobs[n], z_stage(jobs[n]))
            gated.add(n)
        if step[-1]:
            send(step[-1])
            coming = [k[1] for k in steps[at + 1:at + 2] if k[0] == "J"]
            for k in coming:
                if not set(jobs[k].halos) & set(step[-1]):
                    wait_for(k)
        if pipe:
            retire()
        if step[0] == "J":
            pipe.append((n, g))
    if pipe:
        retire()

    @pl.when(me < devices - 1)
    def _():
        for h in halos:
            remote(h).wait_send()


def head_kernel(S, h, w1, b1, w2, b2, y, h_out, Y, sem):
    pass_h = pltpu.make_async_copy(h, h_out, sem.at[0])
    pass_h.start()
    writes = []
    for n, start in enumerate(range(0, ROWS, HEAD_ROWS)):
        rows = slice(start, start + HEAD_ROWS)
        a = jnp.maximum(S[rows], 0.0).astype(BF16)
        m = jnp.maximum(dot(a, w1[...]) + b1[...], 0.0).astype(BF16)
        Y[rows] = dot(m, w2[...]) + b2[...]
        c = pltpu.make_async_copy(Y.at[rows], y.at[rows], sem.at[1 + n])
        c.start()
        writes.append(c)
    pass_h.wait()
    for c in writes:
        c.wait()


def solution(mesh):
    devices = mesh.shape["sp"]
    jobs, halos, steps = plan()
    rows = P(("ens", "sp"), None)

    def local(x, wp, wn, b, wr, ws, w1, b1, w2, b2):
        hbm, near = pl.BlockSpec(memory_space=pltpu.HBM), pl.BlockSpec(memory_space=pltpu.VMEM)
        vmem = lambda *shape: pltpu.VMEM(shape, BF16)
        skip, hidden = pl.pallas_call(
            lambda *refs: stack_kernel(jobs, halos, steps, devices, *refs),
            out_shape=(pltpu.VMEM((ROWS, CH), F32), pltpu.VMEM((ROWS, CH), BF16)),
            in_specs=[hbm] * 6,
            out_specs=(near, near),
            scratch_shapes=[
                vmem(LAYERS, HALO + ROWS, CH), vmem(XROWS, CH), vmem(ROWS, (LAYERS - 1) * CH),
                vmem(LAYERS, 2 * CH, 2 * CH), vmem(LAYERS, CH, CH), vmem(LAYERS * CH, CH),
                pltpu.VMEM((CYCLE, LAYERS // CYCLE, 2 * CH), F32),
                pltpu.SemaphoreType.DMA((LAYERS + 3,)),
                pltpu.SemaphoreType.DMA((len(halos),)), pltpu.SemaphoreType.DMA((len(halos),)),
            ],
            compiler_params=pltpu.CompilerParams(collective_id=0, has_side_effects=True, vmem_limit_bytes=56 * 1024 * 1024),
            name="wavenet_stack",
        )(x, wp.reshape(LAYERS, CH, 2 * CH), wn.reshape(LAYERS, CH, 2 * CH), jnp.swapaxes(b, 0, 1),
          wr.reshape(LAYERS, CH, CH), ws.reshape(LAYERS * CH, CH))
        return pl.pallas_call(
            head_kernel,
            out_shape=(jax.ShapeDtypeStruct((ROWS, CH), F32), jax.ShapeDtypeStruct((ROWS, CH), BF16)),
            in_specs=[near] * 6,
            out_specs=(hbm, hbm),
            scratch_shapes=[pltpu.VMEM((ROWS, CH), F32), pltpu.SemaphoreType.DMA((1 + ROWS // HEAD_ROWS,))],
            compiler_params=pltpu.CompilerParams(vmem_limit_bytes=6 * 1024 * 1024),
            name="wavenet_head",
        )(skip, hidden, w1, b1.reshape(1, CH), w2, b2.reshape(1, CH))

    return jax.shard_map(local, mesh=mesh, in_specs=(rows,) + (P(),) * 9, out_specs=(rows, rows), check_vma=False)
```

```python
import dataclasses

import jax
import jax.numpy as jnp
from jax import lax
from jax.experimental import pallas as pl
from jax.experimental.pallas import tpu as pltpu
from jax.sharding import PartitionSpec as P

F32, BF16 = jnp.float32, jnp.bfloat16
ROWS, CH, LAYERS, CYCLE = 1024, 256, 20, 10
HALO = 256
XROWS = 128
TILE = 256
CUTS = (512, 256)
GROUPS = ()

FIRST_SKIP, FLUSH, FIRST_SEND, END = 128, 159, 160, 255
ORDER = (
    0xc0b0a0807060503010002, 0x1a19171615141211100f0d, 0xa209212304a1201f1e1c1b, 0x9f80189fa31328270e2524,
    0x299fa4269f8382229f811d, 0x389f2c9f8d2a8c8b2b9f8a, 0x3f404a393a443d2da53e37, 0x554b564f4650493b45432e,
    0x52a7a651412f424c5b3c5c, 0x3054535e5d4d4e58574847, 0x3432a9319fa8605f335a59, 0x629f86368561abaa9f8435,
    0x9f93639291908f8e898887, 0xffffffffffffffff659f64,
)


def dil(layer):
    return 2 ** (layer % CYCLE)


@dataclasses.dataclass
class Job:
    layer: int
    start: int
    rows: int
    valid: int
    needs: list = dataclasses.field(default_factory=list)
    halos: list = dataclasses.field(default_factory=list)

    @property
    def end(self):
        return self.start + self.rows


@dataclasses.dataclass
class Halo:
    layer: int
    start: int
    rows: int
    index: int
    needs: list = dataclasses.field(default_factory=list)


def make_jobs():
    jobs = []

    def add(layer, start, rows, valid=None):
        jobs.append(Job(layer, start, rows, start if valid is None else valid))

    for layer in range(7):
        reach = 2 * dil(layer)
        for start in (768, 512, 256):
            add(layer, start, TILE)
        if layer < 6:
            add(layer, 0, TILE, reach - 1)
        else:
            add(layer, 64, TILE - 64, reach - 1)
        low, high = (-128, 64) if layer < 5 else (-64, 64) if layer == 5 else (0, 128)
        add(layer, low, high - low, reach - XROWS)
    for layer in (7, 8, 9, 17, 18):
        for start in (768, 512, 256, 0):
            add(layer, start, TILE)
    for layer in range(10, 17):
        reach, top = 2 * dil(layer), ROWS
        for cut in CUTS + (None,):
            if cut is not None:
                low, valid = cut + 64 * (layer == 16), cut + reach - 1
            elif GROUPS:
                low, valid = 0, 0
            else:
                low, valid = max(-128, min(64 * (layer - 16), 0)) if layer > 14 else -128, reach - XROWS
            count = -(-(top - low) // TILE)
            for left in range(count, 0, -1):
                rows = -(-(top - low) // left // 64) * 64
                top -= rows
                add(layer, top, rows, max(valid, top) if left == 1 else None)
            if cut is not None:
                top = cut + (64 if layer < 16 else 128)
    for start, rows in ((768, 256), (512, 256), (256, 256), (128, 128), (0, 128)):
        add(LAYERS - 1, start, rows)
    return jobs


def make_halos():
    sizes = [(0, 128, 128), (7, 128, 128), (8, 256, 256), (9, 512, 256)]
    if GROUPS:
        sizes += [(layer, max(16, dil(layer)), max(16, dil(layer))) for layer in range(10, 17)]
    else:
        sizes += [(10, 128, 128)]
    sizes += [(17, 128, 128), (18, 256, 256), (19, 512, 128)]
    tops = [(layer, top, chunk) for layer, rows, chunk in sizes for top in range(0, rows, chunk)]
    return [Halo(layer, -top - chunk, chunk, index) for index, (layer, top, chunk) in enumerate(tops)]


def plan():
    jobs, halos = make_jobs(), make_halos()
    sent = {h.layer for h in halos}

    def cover(layer, low, high):
        found, want = [], set(range(low, high)) if layer else set()
        for n, j in enumerate(jobs):
            have = want & set(range(max(j.valid, j.start), j.end)) if j.layer == layer - 1 else set()
            if have:
                found.append(n)
                want -= have
        assert not want, (layer, low, high)
        return found

    for n, j in enumerate(jobs):
        for back in (0, dil(j.layer)):
            low, high = j.valid - back, j.end - back
            inner = low
            if low < 0 and j.layer in sent:
                inner = 0
                j.halos += [h.index for h in halos if h.layer == j.layer and h.start < high and h.start + h.rows > low and h.index not in j.halos]
            j.needs += [k for k in cover(j.layer, inner, high) if k not in j.needs]
        j.needs += [k for k, q in enumerate(jobs) if q.layer == j.layer and k != n and k not in j.needs
                    and q.start < j.end and q.valid > max(j.start, q.start, j.valid)]
    for h in halos:
        h.needs = cover(h.layer, ROWS + h.start, ROWS + h.start + h.rows)
    for group in GROUPS:
        union = sorted({k for h in halos if h.layer in group for k in h.needs})
        for h in halos:
            if h.layer in group:
                h.needs = union

    pieces = [(layer, min(2, LAYERS - 1 - layer), start) for start in (512, 0) for layer in range(0, LAYERS - 1, 2)]
    steps = []
    for code in [word >> 8 * k & 255 for word in ORDER for k in range(11)]:
        if code >= FIRST_SEND and code != END:
            steps[-1][-1].append(code - FIRST_SEND)
        elif code == FLUSH:
            steps.append(("F", []))
        elif FIRST_SKIP <= code < FLUSH:
            steps.append(("S", pieces[code - FIRST_SKIP]))
        elif code < FIRST_SKIP:
            steps.append(("J", code, []))
    return jobs, halos, steps


HEAD_ROWS = 256
WEIGHT_WAITS = (0, 1, 4, 9, 20)


def dot(a, b):
    return jnp.dot(a, b, preferred_element_type=F32)


def stack_kernel(jobs, halos, steps, devices, x, wp, wn, b, wr, ws, S, h_out,
                 H, G, W, WR, WS, B, wsem, send_sem, recv_sem, *lands):
    me = lax.axis_index("sp")
    first = me == 0
    land = dict(zip(dict.fromkeys(h.layer for h in halos), lands))

    load_x = pltpu.make_async_copy(x, H.at[0, HALO:HALO + ROWS], wsem.at[LAYERS + 1])
    load_b = pltpu.make_async_copy(b, B, wsem.at[LAYERS])
    layer_loads = []
    for layer in range(LAYERS):
        layer_loads.append([pltpu.make_async_copy(wp.at[layer], W.at[layer, 0:CH], wsem.at[layer]),
                            pltpu.make_async_copy(wn.at[layer], W.at[layer, CH:2 * CH], wsem.at[layer]),
                            pltpu.make_async_copy(wr.at[layer], WR.at[layer], wsem.at[layer])])
    load_skip = pltpu.make_async_copy(ws, WS, wsem.at[LAYERS + 2])
    for c in [load_x] + layer_loads[0] + [load_b]:
        c.start()
    for group in layer_loads[1:]:
        for c in group:
            c.start()
    load_skip.start()

    @pl.when(first)
    def _():
        for ref in lands:
            ref[...] = jnp.zeros_like(ref)

    barrier = pltpu.get_barrier_semaphore()

    @pl.when(me > 0)
    def _():
        pl.semaphore_signal(barrier, inc=1, device_id={"sp": me - 1}, device_id_type=pl.DeviceIdType.MESH)

    @pl.when(me < devices - 1)
    def _():
        pl.semaphore_wait(barrier, 1)

    def remote(h):
        src = H.at[h.layer, HALO + ROWS + h.start:HALO + ROWS + h.start + h.rows]
        at = land[h.layer].shape[0] + h.start
        dst = land[h.layer].at[at:at + h.rows]
        return pltpu.make_async_remote_copy(
            src_ref=src, dst_ref=dst, send_sem=send_sem.at[h.index], recv_sem=recv_sem.at[h.index],
            device_id={"sp": lax.rem(me + 1, devices)}, device_id_type=pl.DeviceIdType.MESH)

    finished, gated, arrived, weighed, summed = set(), set(), set(), set(), set()

    def wait_weights(layer):
        if layer not in weighed:
            low = max(k for k in WEIGHT_WAITS if k <= layer)
            high = min(k for k in WEIGHT_WAITS if k > layer)
            for k in range(low, high):
                weighed.add(k)
                for c in layer_loads[k]:
                    c.wait()
            if high == LAYERS:
                weighed.add("skip")
                load_skip.wait()

    def wait_for(n):
        wait_weights(jobs[n].layer)
        wait_halos(n)

    def wait_halos(n):
        if jobs[n].halos:
            wait_weights(LAYERS - 1)
        for h in jobs[n].halos:
            if h not in arrived:
                arrived.add(h)
                pl.when(me > 0)(remote(halos[h]).wait_recv)
                if halos[h].layer % CYCLE == 0:
                    H[halos[h].layer, HALO - XROWS:HALO] = land[halos[h].layer][...]

    def send(which):
        for h in which:
            assert finished.issuperset(halos[h].needs)
            pl.when(me < devices - 1)(remote(halos[h]).start)

    def z_stage(job):
        low, high, d = job.start, job.end, dil(job.layer)
        now = H[job.layer, HALO + low:HALO + high]
        if job.halos and job.layer % CYCLE:
            past = land[job.layer][low:min(high, d)]
            if high > d:
                past = jnp.concatenate([past, H[job.layer, HALO:HALO + high - d]], axis=0)
        else:
            past = H[job.layer, HALO + low - d:HALO + high - d]
        return dot(jnp.concatenate([past, now], axis=1), W[job.layer])

    def gate_stage(job, z):
        z = z + B[job.layer % CYCLE, job.layer // CYCLE:job.layer // CYCLE + 1]
        t = jnp.tanh(z[:, :CH])
        u = jnp.tanh(0.5 * z[:, CH:])
        g = (0.5 * (t * u + t)).astype(BF16)
        cut = max(-job.start, 0)
        if cut < job.rows and job.layer < LAYERS - 1:
            G[job.start + cut:job.end, job.layer * CH:(job.layer + 1) * CH] = g[cut:]
        return g

    def fin_stage(n, g):
        job = jobs[n]
        at = HALO + job.start
        new = (H[job.layer, at:at + job.rows].astype(F32) + dot(g, WR[job.layer])).astype(BF16)
        if job.layer == LAYERS - 1:
            h_out[job.start:job.end] = new
            add_skip(slice(job.start, job.end), dot(g, WS[(LAYERS - 1) * CH:]))
        elif job.start < 0:
            cut = min(-job.start, job.rows)
            H[job.layer + 1, at:at + cut] = jnp.where(first, jnp.zeros((cut, CH), BF16), new[:cut])
            if cut < job.rows:
                H[job.layer + 1, at + cut:at + job.rows] = new[cut:]
        else:
            H[job.layer + 1, at:at + job.rows] = new
        finished.add(n)

    def add_skip(rows, part):
        S[rows] = S[rows] + part if rows.start // TILE in summed else part

    def skip_stage(layer, count, start):
        for low in (start, start + TILE):
            rows = slice(low, low + TILE)
            add_skip(rows, dot(G[rows, layer * CH:(layer + count) * CH], WS[layer * CH:(layer + count) * CH]))
            summed.add(low // TILE)

    pipe = []

    def retire():
        n, g = pipe.pop()
        fin_stage(n, g)

    load_x.wait()
    send([n for n, h in enumerate(halos) if not h.layer])
    load_b.wait()
    for at, step in enumerate(steps):
        if step[0] == "S":
            assert "skip" in weighed
            skip_stage(*step[1])
            continue
        if step[0] == "J":
            n = step[1]
            assert finished.issuperset(jobs[n].needs), jobs[n]
            wait_for(n)
            g = gate_stage(jobs[n], z_stage(jobs[n]))
            gated.add(n)
        if pipe:
            retire()
        if step[-1]:
            send(step[-1])
            for k in [k[1] for k in steps[at + 1:at + 2] if k[0] == "J"]:
                wait_for(k)
        if step[0] == "J":
            pipe.append((n, g))
    if pipe:
        retire()

    @pl.when(me < devices - 1)
    def _():
        for h in halos:
            remote(h).wait_send()


def head_kernel(S, h, w1, b1, w2, b2, y, h_out, Y, sem):
    pass_h = pltpu.make_async_copy(h, h_out, sem.at[0])
    pass_h.start()
    writes = []
    for n, start in enumerate(range(0, ROWS, HEAD_ROWS)):
        rows = slice(start, start + HEAD_ROWS)
        a = jnp.maximum(S[rows], 0.0).astype(BF16)
        m = jnp.maximum(dot(a, w1[...]) + b1[...], 0.0).astype(BF16)
        Y[rows] = dot(m, w2[...]) + b2[...]
        c = pltpu.make_async_copy(Y.at[rows], y.at[rows], sem.at[1 + n])
        c.start()
        writes.append(c)
    pass_h.wait()
    for c in writes:
        c.wait()


def solution(mesh):
    devices = mesh.shape["sp"]
    jobs, halos, steps = plan()
    tall = {h.layer: max(-k.start for k in halos if k.layer == h.layer) for h in halos}
    rows = P(("ens", "sp"), None)

    def local(x, wp, wn, b, wr, ws, w1, b1, w2, b2):
        hbm, near = pl.BlockSpec(memory_space=pltpu.HBM), pl.BlockSpec(memory_space=pltpu.VMEM)
        vmem = lambda *shape: pltpu.VMEM(shape, BF16)
        skip, hidden = pl.pallas_call(
            lambda *refs: stack_kernel(jobs, halos, steps, devices, *refs),
            out_shape=(pltpu.VMEM((ROWS, CH), F32), pltpu.VMEM((ROWS, CH), BF16)),
            in_specs=[hbm] * 6,
            out_specs=(near, near),
            scratch_shapes=[
                vmem(LAYERS, HALO + ROWS, CH), vmem(ROWS, (LAYERS - 1) * CH),
                vmem(LAYERS, 2 * CH, 2 * CH), vmem(LAYERS, CH, CH), vmem(LAYERS * CH, CH),
                pltpu.VMEM((CYCLE, LAYERS // CYCLE, 2 * CH), F32),
                pltpu.SemaphoreType.DMA((LAYERS + 3,)),
                pltpu.SemaphoreType.DMA((len(halos),)), pltpu.SemaphoreType.DMA((len(halos),)),
            ] + [vmem(n, CH) for n in tall.values()],
            compiler_params=pltpu.CompilerParams(collective_id=0, has_side_effects=True, vmem_limit_bytes=56 * 1024 * 1024),
            name="wavenet_stack",
        )(x, wp.reshape(LAYERS, CH, 2 * CH), wn.reshape(LAYERS, CH, 2 * CH), jnp.swapaxes(b, 0, 1),
          wr.reshape(LAYERS, CH, CH), ws.reshape(LAYERS * CH, CH))
        return pl.pallas_call(
            head_kernel,
            out_shape=(jax.ShapeDtypeStruct((ROWS, CH), F32), jax.ShapeDtypeStruct((ROWS, CH), BF16)),
            in_specs=[near] * 6,
            out_specs=(hbm, hbm),
            scratch_shapes=[pltpu.VMEM((ROWS, CH), F32), pltpu.SemaphoreType.DMA((1 + ROWS // HEAD_ROWS,))],
            compiler_params=pltpu.CompilerParams(vmem_limit_bytes=6 * 1024 * 1024),
            name="wavenet_head",
        )(skip, hidden, w1, b1.reshape(1, CH), w2, b2.reshape(1, CH))

    return jax.shard_map(local, mesh=mesh, in_specs=(rows,) + (P(),) * 9, out_specs=(rows, rows), check_vma=False)
```

```python
import dataclasses

import jax
import jax.numpy as jnp
from jax import lax
from jax.experimental import pallas as pl
from jax.experimental.pallas import tpu as pltpu
from jax.sharding import PartitionSpec as P

F32, BF16 = jnp.float32, jnp.bfloat16
ROWS, CH, LAYERS, CYCLE = 1024, 256, 20, 10
HALO = 256
XROWS = 128
TILE = 256
CUTS = (512, 256)
GROUPS = ()

FIRST_SKIP, FLUSH, FIRST_SEND, END = 128, 159, 160, 255
ORDER = (
    0xc0b0a0807060503010002, 0x1a19171615141211100f0d, 0xa209212304a1201f1e1c1b, 0x9f80189fa31328270e2524,
    0x299fa4269f8382229f811d, 0x389f2c9f8d2a8c8b2b9f8a, 0x3f404a393a443d2da53e37, 0x554b564f4650493b45432e,
    0x52a7a651412f424c5b3c5c, 0x3054535e5d4d4e58574847, 0x3432a9319fa8605f335a59, 0x629f86368561abaa9f8435,
    0x9f93639291908f8e898887, 0xffffffffffffffff659f64,
)


def dil(layer):
    return 2 ** (layer % CYCLE)


@dataclasses.dataclass
class Job:
    layer: int
    start: int
    rows: int
    valid: int
    needs: list = dataclasses.field(default_factory=list)
    halos: list = dataclasses.field(default_factory=list)

    @property
    def end(self):
        return self.start + self.rows


@dataclasses.dataclass
class Halo:
    layer: int
    start: int
    rows: int
    index: int
    needs: list = dataclasses.field(default_factory=list)


def make_jobs():
    jobs = []

    def add(layer, start, rows, valid=None):
        jobs.append(Job(layer, start, rows, start if valid is None else valid))

    for layer in range(7):
        reach = 2 * dil(layer)
        for start in (768, 512, 256):
            add(layer, start, TILE)
        if layer < 6:
            add(layer, 0, TILE, reach - 1)
        else:
            add(layer, 64, TILE - 64, reach - 1)
        low, high = (-128, 64) if layer < 5 else (-64, 64) if layer == 5 else (0, 128)
        add(layer, low, high - low, reach - XROWS)
    for layer in (7, 8, 9, 17, 18):
        for start in (768, 512, 256, 0):
            add(layer, start, TILE)
    for layer in range(10, 17):
        reach, top = 2 * dil(layer), ROWS
        for cut in CUTS + (None,):
            if cut is not None:
                low, valid = cut + 64 * (layer == 16), cut + reach - 1
            elif GROUPS:
                low, valid = 0, 0
            else:
                low, valid = max(-128, min(64 * (layer - 16), 0)) if layer > 14 else -128, reach - XROWS
            count = -(-(top - low) // TILE)
            for left in range(count, 0, -1):
                rows = -(-(top - low) // left // 64) * 64
                top -= rows
                add(layer, top, rows, max(valid, top) if left == 1 else None)
            if cut is not None:
                top = cut + (64 if layer < 16 else 128)
    for start, rows in ((768, 256), (512, 256), (256, 256), (128, 128), (0, 128)):
        add(LAYERS - 1, start, rows)
    return jobs


def make_halos():
    sizes = [(0, 128, 128), (7, 128, 128), (8, 256, 256), (9, 512, 256)]
    if GROUPS:
        sizes += [(layer, max(16, dil(layer)), max(16, dil(layer))) for layer in range(10, 17)]
    else:
        sizes += [(10, 128, 128)]
    sizes += [(17, 128, 128), (18, 256, 256), (19, 512, 128)]
    tops = [(layer, top, chunk) for layer, rows, chunk in sizes for top in range(0, rows, chunk)]
    return [Halo(layer, -top - chunk, chunk, index) for index, (layer, top, chunk) in enumerate(tops)]


def plan():
    jobs, halos = make_jobs(), make_halos()
    sent = {h.layer for h in halos}

    def cover(layer, low, high):
        found, want = [], set(range(low, high)) if layer else set()
        for n, j in enumerate(jobs):
            have = want & set(range(max(j.valid, j.start), j.end)) if j.layer == layer - 1 else set()
            if have:
                found.append(n)
                want -= have
        assert not want, (layer, low, high)
        return found

    for n, j in enumerate(jobs):
        for back in (0, dil(j.layer)):
            low, high = j.valid - back, j.end - back
            inner = low
            if low < 0 and j.layer in sent:
                inner = 0
                j.halos += [h.index for h in halos if h.layer == j.layer and h.start < high and h.start + h.rows > low and h.index not in j.halos]
            j.needs += [k for k in cover(j.layer, inner, high) if k not in j.needs]
        j.needs += [k for k, q in enumerate(jobs) if q.layer == j.layer and k != n and k not in j.needs
                    and q.start < j.end and q.valid > max(j.start, q.start, j.valid)]
    for h in halos:
        h.needs = cover(h.layer, ROWS + h.start, ROWS + h.start + h.rows)
    for group in GROUPS:
        union = sorted({k for h in halos if h.layer in group for k in h.needs})
        for h in halos:
            if h.layer in group:
                h.needs = union

    pieces = [(layer, min(2, LAYERS - 1 - layer), start) for start in (512, 0) for layer in range(0, LAYERS - 1, 2)]
    steps = []
    for code in [word >> 8 * k & 255 for word in ORDER for k in range(11)]:
        if code >= FIRST_SEND and code != END:
            steps[-1][-1].append(code - FIRST_SEND)
        elif code == FLUSH:
            steps.append(("F", []))
        elif FIRST_SKIP <= code < FLUSH:
            steps.append(("S", pieces[code - FIRST_SKIP]))
        elif code < FIRST_SKIP:
            steps.append(("J", code, []))
    return jobs, halos, steps


HEAD_ROWS = 256
ENTER = 1
WEIGHT_WAITS = (0, 1, 4, 9, 20)


def dot(a, b):
    return jnp.dot(a, b, preferred_element_type=F32)


def stack_kernel(jobs, halos, steps, devices, x, wp, wn, b, wr, ws, S, h_out,
                 H, G, W, WR, WS, B, wsem, send_sem, recv_sem, *lands):
    me = lax.axis_index("sp")
    first = me == 0
    land = dict(zip(dict.fromkeys(h.layer for h in halos), lands))

    load_x = pltpu.make_async_copy(x, H.at[0, HALO:HALO + ROWS], wsem.at[LAYERS + 1])
    load_b = pltpu.make_async_copy(b, B, wsem.at[LAYERS])
    layer_loads = []
    for layer in range(LAYERS):
        layer_loads.append([pltpu.make_async_copy(wp.at[layer], W.at[layer, 0:CH], wsem.at[layer]),
                            pltpu.make_async_copy(wn.at[layer], W.at[layer, CH:2 * CH], wsem.at[layer]),
                            pltpu.make_async_copy(wr.at[layer], WR.at[layer], wsem.at[layer])])
    load_skip = pltpu.make_async_copy(ws, WS, wsem.at[LAYERS + 2])
    for c in [load_x] + layer_loads[0] + [load_b]:
        c.start()
    for group in layer_loads[1:]:
        for c in group:
            c.start()
    load_skip.start()

    @pl.when(first)
    def _():
        for ref in lands:
            ref[...] = jnp.zeros_like(ref)

    barrier = pltpu.get_barrier_semaphore()

    @pl.when(me > 0)
    def _():
        pl.semaphore_signal(barrier, inc=1, device_id={"sp": me - 1}, device_id_type=pl.DeviceIdType.MESH)

    def remote(h):
        src = H.at[h.layer, HALO + ROWS + h.start:HALO + ROWS + h.start + h.rows]
        at = land[h.layer].shape[0] + h.start
        dst = land[h.layer].at[at:at + h.rows]
        return pltpu.make_async_remote_copy(
            src_ref=src, dst_ref=dst, send_sem=send_sem.at[h.index], recv_sem=recv_sem.at[h.index],
            device_id={"sp": lax.rem(me + 1, devices)}, device_id_type=pl.DeviceIdType.MESH)

    finished, gated, arrived, weighed, summed = set(), set(), set(), set(), set()

    def wait_weights(layer):
        if layer not in weighed:
            low = max(k for k in WEIGHT_WAITS if k <= layer)
            high = min(k for k in WEIGHT_WAITS if k > layer)
            if low == ENTER:
                enter()
            for k in range(low, high):
                weighed.add(k)
                for c in layer_loads[k]:
                    c.wait()
            if high == LAYERS:
                weighed.add("skip")
                load_skip.wait()

    def enter():
        @pl.when(me < devices - 1)
        def _():
            pl.semaphore_wait(barrier, 1)
        send([n for n, h in enumerate(halos) if not h.layer])

    def wait_for(n):
        wait_weights(jobs[n].layer)
        wait_halos(n)

    def wait_halos(n):
        if jobs[n].halos:
            wait_weights(LAYERS - 1)
        for h in jobs[n].halos:
            if h not in arrived:
                arrived.add(h)
                pl.when(me > 0)(remote(halos[h]).wait_recv)
                if halos[h].layer % CYCLE == 0:
                    H[halos[h].layer, HALO - XROWS:HALO] = land[halos[h].layer][...]

    def send(which):
        for h in which:
            assert finished.issuperset(halos[h].needs)
            pl.when(me < devices - 1)(remote(halos[h]).start)

    def z_stage(job):
        low, high, d = job.start, job.end, dil(job.layer)
        now = H[job.layer, HALO + low:HALO + high]
        if job.halos and job.layer % CYCLE:
            past = land[job.layer][low:min(high, d)]
            if high > d:
                past = jnp.concatenate([past, H[job.layer, HALO:HALO + high - d]], axis=0)
        else:
            past = H[job.layer, HALO + low - d:HALO + high - d]
        return dot(jnp.concatenate([past, now], axis=1), W[job.layer])

    def gate_stage(job, z):
        z = z + B[job.layer % CYCLE, job.layer // CYCLE:job.layer // CYCLE + 1]
        t = jnp.tanh(z[:, :CH])
        u = jnp.tanh(0.5 * z[:, CH:])
        g = (0.5 * (t * u + t)).astype(BF16)
        cut = max(-job.start, 0)
        if cut < job.rows and job.layer < LAYERS - 1:
            G[job.start + cut:job.end, job.layer * CH:(job.layer + 1) * CH] = g[cut:]
        return g

    def fin_stage(n, g):
        job = jobs[n]
        at = HALO + job.start
        new = (H[job.layer, at:at + job.rows].astype(F32) + dot(g, WR[job.layer])).astype(BF16)
        if job.layer == LAYERS - 1:
            h_out[job.start:job.end] = new
            add_skip(slice(job.start, job.end), dot(g, WS[(LAYERS - 1) * CH:]))
        elif job.start < 0:
            cut = min(-job.start, job.rows)
            H[job.layer + 1, at:at + cut] = jnp.where(first, jnp.zeros((cut, CH), BF16), new[:cut])
            if cut < job.rows:
                H[job.layer + 1, at + cut:at + job.rows] = new[cut:]
        else:
            H[job.layer + 1, at:at + job.rows] = new
        finished.add(n)

    def add_skip(rows, part):
        S[rows] = S[rows] + part if rows.start // TILE in summed else part

    def skip_stage(layer, count, start):
        for low in (start, start + TILE):
            rows = slice(low, low + TILE)
            add_skip(rows, dot(G[rows, layer * CH:(layer + count) * CH], WS[layer * CH:(layer + count) * CH]))
            summed.add(low // TILE)

    pipe = []

    def retire():
        n, g = pipe.pop()
        fin_stage(n, g)

    load_x.wait()
    load_b.wait()
    for at, step in enumerate(steps):
        if step[0] == "S":
            assert "skip" in weighed
            skip_stage(*step[1])
            continue
        if step[0] == "J":
            n = step[1]
            assert finished.issuperset(jobs[n].needs), jobs[n]
            wait_for(n)
            g = gate_stage(jobs[n], z_stage(jobs[n]))
            gated.add(n)
        if pipe:
            retire()
        if step[-1]:
            send(step[-1])
            for k in [k[1] for k in steps[at + 1:at + 2] if k[0] == "J"]:
                wait_for(k)
        if step[0] == "J":
            pipe.append((n, g))
    if pipe:
        retire()

    @pl.when(me < devices - 1)
    def _():
        for h in halos:
            remote(h).wait_send()


def head_kernel(S, h, w1, b1, w2, b2, y, h_out, Y, sem):
    pass_h = pltpu.make_async_copy(h, h_out, sem.at[0])
    pass_h.start()
    writes = []
    for n, start in enumerate(range(0, ROWS, HEAD_ROWS)):
        rows = slice(start, start + HEAD_ROWS)
        a = jnp.maximum(S[rows], 0.0).astype(BF16)
        m = jnp.maximum(dot(a, w1[...]) + b1[...], 0.0).astype(BF16)
        Y[rows] = dot(m, w2[...]) + b2[...]
        c = pltpu.make_async_copy(Y.at[rows], y.at[rows], sem.at[1 + n])
        c.start()
        writes.append(c)
    pass_h.wait()
    for c in writes:
        c.wait()


def solution(mesh):
    devices = mesh.shape["sp"]
    jobs, halos, steps = plan()
    tall = {h.layer: max(-k.start for k in halos if k.layer == h.layer) for h in halos}
    rows = P(("ens", "sp"), None)

    def local(x, wp, wn, b, wr, ws, w1, b1, w2, b2):
        hbm, near = pl.BlockSpec(memory_space=pltpu.HBM), pl.BlockSpec(memory_space=pltpu.VMEM)
        vmem = lambda *shape: pltpu.VMEM(shape, BF16)
        skip, hidden = pl.pallas_call(
            lambda *refs: stack_kernel(jobs, halos, steps, devices, *refs),
            out_shape=(pltpu.VMEM((ROWS, CH), F32), pltpu.VMEM((ROWS, CH), BF16)),
            in_specs=[hbm] * 6,
            out_specs=(near, near),
            scratch_shapes=[
                vmem(LAYERS, HALO + ROWS, CH), vmem(ROWS, (LAYERS - 1) * CH),
                vmem(LAYERS, 2 * CH, 2 * CH), vmem(LAYERS, CH, CH), vmem(LAYERS * CH, CH),
                pltpu.VMEM((CYCLE, LAYERS // CYCLE, 2 * CH), F32),
                pltpu.SemaphoreType.DMA((LAYERS + 3,)),
                pltpu.SemaphoreType.DMA((len(halos),)), pltpu.SemaphoreType.DMA((len(halos),)),
            ] + [vmem(n, CH) for n in tall.values()],
            compiler_params=pltpu.CompilerParams(collective_id=0, has_side_effects=True, vmem_limit_bytes=56 * 1024 * 1024),
            name="wavenet_stack",
        )(x, wp.reshape(LAYERS, CH, 2 * CH), wn.reshape(LAYERS, CH, 2 * CH), jnp.swapaxes(b, 0, 1),
          wr.reshape(LAYERS, CH, CH), ws.reshape(LAYERS * CH, CH))
        return pl.pallas_call(
            head_kernel,
            out_shape=(jax.ShapeDtypeStruct((ROWS, CH), F32), jax.ShapeDtypeStruct((ROWS, CH), BF16)),
            in_specs=[near] * 6,
            out_specs=(hbm, hbm),
            scratch_shapes=[pltpu.VMEM((ROWS, CH), F32), pltpu.SemaphoreType.DMA((1 + ROWS // HEAD_ROWS,))],
            compiler_params=pltpu.CompilerParams(vmem_limit_bytes=6 * 1024 * 1024),
            name="wavenet_head",
        )(skip, hidden, w1, b1.reshape(1, CH), w2, b2.reshape(1, CH))

    return jax.shard_map(local, mesh=mesh, in_specs=(rows,) + (P(),) * 9, out_specs=(rows, rows), check_vma=False)
```

```python
import dataclasses

import jax
import jax.numpy as jnp
from jax import lax
from jax.experimental import pallas as pl
from jax.experimental.pallas import tpu as pltpu
from jax.sharding import PartitionSpec as P

F32, BF16 = jnp.float32, jnp.bfloat16
ROWS, CH, LAYERS, CYCLE = 1024, 256, 20, 10
HALO = 256
XROWS = 128
TILE = 256
CUTS = (512, 256)
GROUPS = ()

FIRST_SKIP, FLUSH, FIRST_SEND, END = 128, 159, 160, 255
ORDER = (
    0xc0b0a0807060503010002, 0x1a19171615141211100f0d, 0xa209212304a1201f1e1c1b, 0x1d9f80189f1328270e2524,
    0x299fa4a3269f8382229f81, 0x389f2c9f8d2a8c8b2b9f8a, 0x3f404a393a443d2da53e37, 0x554b564f4650493b45432e,
    0x52a7a651412f424c5b3c5c, 0x3054535e5d4d4e58574847, 0x3432a9319fa8605f335a59, 0x629f86368561abaa9f8435,
    0x9f93639291908f8e898887, 0xffffffffffffffff659f64,
)


def dil(layer):
    return 2 ** (layer % CYCLE)


@dataclasses.dataclass
class Job:
    layer: int
    start: int
    rows: int
    valid: int
    needs: list = dataclasses.field(default_factory=list)
    halos: list = dataclasses.field(default_factory=list)

    @property
    def end(self):
        return self.start + self.rows


@dataclasses.dataclass
class Halo:
    layer: int
    start: int
    rows: int
    index: int
    needs: list = dataclasses.field(default_factory=list)


def make_jobs():
    jobs = []

    def add(layer, start, rows, valid=None):
        jobs.append(Job(layer, start, rows, start if valid is None else valid))

    for layer in range(7):
        reach = 2 * dil(layer)
        for start in (768, 512, 256):
            add(layer, start, TILE)
        if layer < 6:
            add(layer, 0, TILE, reach - 1)
        else:
            add(layer, 64, TILE - 64, reach - 1)
        low, high = (-128, 64) if layer < 5 else (-64, 64) if layer == 5 else (0, 128)
        add(layer, low, high - low, reach - XROWS)
    for layer in (7, 8, 9, 17, 18):
        for start in (768, 512, 256, 0):
            add(layer, start, TILE)
    for layer in range(10, 17):
        reach, top = 2 * dil(layer), ROWS
        for cut in CUTS + (None,):
            if cut is not None:
                low, valid = cut + 64 * (layer == 16), cut + reach - 1
            elif GROUPS:
                low, valid = 0, 0
            else:
                low, valid = max(-128, min(64 * (layer - 16), 0)) if layer > 14 else -128, reach - XROWS
            count = -(-(top - low) // TILE)
            for left in range(count, 0, -1):
                rows = -(-(top - low) // left // 64) * 64
                top -= rows
                add(layer, top, rows, max(valid, top) if left == 1 else None)
            if cut is not None:
                top = cut + (64 if layer < 16 else 128)
    for start, rows in ((768, 256), (512, 256), (256, 256), (128, 128), (0, 128)):
        add(LAYERS - 1, start, rows)
    return jobs


def make_halos():
    sizes = [(0, 128, 128), (7, 128, 128), (8, 256, 256), (9, 512, 256)]
    if GROUPS:
        sizes += [(layer, max(16, dil(layer)), max(16, dil(layer))) for layer in range(10, 17)]
    else:
        sizes += [(10, 128, 128)]
    sizes += [(17, 128, 128), (18, 256, 256), (19, 512, 128)]
    tops = [(layer, top, chunk) for layer, rows, chunk in sizes for top in range(0, rows, chunk)]
    return [Halo(layer, -top - chunk, chunk, index) for index, (layer, top, chunk) in enumerate(tops)]


def plan():
    jobs, halos = make_jobs(), make_halos()
    sent = {h.layer for h in halos}

    def cover(layer, low, high):
        found, want = [], set(range(low, high)) if layer else set()
        for n, j in enumerate(jobs):
            have = want & set(range(max(j.valid, j.start), j.end)) if j.layer == layer - 1 else set()
            if have:
                found.append(n)
                want -= have
        assert not want, (layer, low, high)
        return found

    for n, j in enumerate(jobs):
        for back in (0, dil(j.layer)):
            low, high = j.valid - back, j.end - back
            inner = low
            if low < 0 and j.layer in sent:
                inner = 0
                j.halos += [h.index for h in halos if h.layer == j.layer and h.start < high and h.start + h.rows > low and h.index not in j.halos]
            j.needs += [k for k in cover(j.layer, inner, high) if k not in j.needs]
        j.needs += [k for k, q in enumerate(jobs) if q.layer == j.layer and k != n and k not in j.needs
                    and q.start < j.end and q.valid > max(j.start, q.start, j.valid)]
    for h in halos:
        h.needs = cover(h.layer, ROWS + h.start, ROWS + h.start + h.rows)
    for group in GROUPS:
        union = sorted({k for h in halos if h.layer in group for k in h.needs})
        for h in halos:
            if h.layer in group:
                h.needs = union

    pieces = [(layer, min(2, LAYERS - 1 - layer), start) for start in (512, 0) for layer in range(0, LAYERS - 1, 2)]
    steps = []
    for code in [word >> 8 * k & 255 for word in ORDER for k in range(11)]:
        if code >= FIRST_SEND and code != END:
            steps[-1][-1].append(code - FIRST_SEND)
        elif code == FLUSH:
            steps.append(("F", []))
        elif FIRST_SKIP <= code < FLUSH:
            steps.append(("S", pieces[code - FIRST_SKIP]))
        elif code < FIRST_SKIP:
            steps.append(("J", code, []))
    return jobs, halos, steps


HEAD_ROWS = 256
ENTER = 1
WEIGHT_WAITS = (0, 1, 4, 9, 20)


def dot(a, b):
    return jnp.dot(a, b, preferred_element_type=F32)


def stack_kernel(jobs, halos, steps, devices, x, wp, wn, b, wr, ws, S, h_out,
                 H, G, W, WR, WS, B, wsem, send_sem, recv_sem, *lands):
    me = lax.axis_index("sp")
    first = me == 0
    land = dict(zip(dict.fromkeys(h.layer for h in halos), lands))

    load_x = pltpu.make_async_copy(x, H.at[0, HALO:HALO + ROWS], wsem.at[LAYERS + 1])
    load_b = pltpu.make_async_copy(b, B, wsem.at[LAYERS])
    layer_loads = []
    for layer in range(LAYERS):
        layer_loads.append([pltpu.make_async_copy(wp.at[layer], W.at[layer, 0:CH], wsem.at[layer]),
                            pltpu.make_async_copy(wn.at[layer], W.at[layer, CH:2 * CH], wsem.at[layer]),
                            pltpu.make_async_copy(wr.at[layer], WR.at[layer], wsem.at[layer])])
    load_skip = pltpu.make_async_copy(ws, WS, wsem.at[LAYERS + 2])
    for c in [load_x] + layer_loads[0] + [load_b]:
        c.start()
    for group in layer_loads[1:]:
        for c in group:
            c.start()
    load_skip.start()

    @pl.when(first)
    def _():
        for ref in lands:
            ref[...] = jnp.zeros_like(ref)

    barrier = pltpu.get_barrier_semaphore()

    @pl.when(me > 0)
    def _():
        pl.semaphore_signal(barrier, inc=1, device_id={"sp": me - 1}, device_id_type=pl.DeviceIdType.MESH)

    def remote(h):
        src = H.at[h.layer, HALO + ROWS + h.start:HALO + ROWS + h.start + h.rows]
        at = land[h.layer].shape[0] + h.start
        dst = land[h.layer].at[at:at + h.rows]
        return pltpu.make_async_remote_copy(
            src_ref=src, dst_ref=dst, send_sem=send_sem.at[h.index], recv_sem=recv_sem.at[h.index],
            device_id={"sp": lax.rem(me + 1, devices)}, device_id_type=pl.DeviceIdType.MESH)

    finished, gated, arrived, weighed, summed = set(), set(), set(), set(), set()

    def wait_weights(layer):
        if layer not in weighed:
            low = max(k for k in WEIGHT_WAITS if k <= layer)
            high = min(k for k in WEIGHT_WAITS if k > layer)
            if low == ENTER:
                enter()
            for k in range(low, high):
                weighed.add(k)
                for c in layer_loads[k]:
                    c.wait()
            if high == LAYERS:
                weighed.add("skip")
                load_skip.wait()

    def enter():
        @pl.when(me < devices - 1)
        def _():
            pl.semaphore_wait(barrier, 1)
        send([n for n, h in enumerate(halos) if not h.layer])

    def wait_for(n):
        wait_weights(jobs[n].layer)
        wait_halos(n)

    def wait_halos(n):
        if jobs[n].halos:
            wait_weights(LAYERS - 1)
        for h in jobs[n].halos:
            if h not in arrived:
                arrived.add(h)
                pl.when(me > 0)(remote(halos[h]).wait_recv)
                if halos[h].layer % CYCLE == 0:
                    H[halos[h].layer, HALO - XROWS:HALO] = land[halos[h].layer][...]

    def send(which):
        for h in which:
            assert finished.issuperset(halos[h].needs)
            pl.when(me < devices - 1)(remote(halos[h]).start)

    def z_stage(job):
        low, high, d = job.start, job.end, dil(job.layer)
        now = H[job.layer, HALO + low:HALO + high]
        if job.halos and job.layer % CYCLE:
            past = land[job.layer][low:min(high, d)]
            if high > d:
                past = jnp.concatenate([past, H[job.layer, HALO:HALO + high - d]], axis=0)
        else:
            past = H[job.layer, HALO + low - d:HALO + high - d]
        return dot(jnp.concatenate([past, now], axis=1), W[job.layer])

    def gate_stage(job, z):
        z = z + B[job.layer % CYCLE, job.layer // CYCLE:job.layer // CYCLE + 1]
        t = jnp.tanh(z[:, :CH])
        u = jnp.tanh(0.5 * z[:, CH:])
        g = (0.5 * (t * u + t)).astype(BF16)
        cut = max(-job.start, 0)
        if cut < job.rows and job.layer < LAYERS - 1:
            G[job.start + cut:job.end, job.layer * CH:(job.layer + 1) * CH] = g[cut:]
        return g

    def fin_stage(n, g):
        job = jobs[n]
        at = HALO + job.start
        new = (H[job.layer, at:at + job.rows].astype(F32) + dot(g, WR[job.layer])).astype(BF16)
        if job.layer == LAYERS - 1:
            h_out[job.start:job.end] = new
            add_skip(slice(job.start, job.end), dot(g, WS[(LAYERS - 1) * CH:]))
        elif job.start < 0:
            cut = min(-job.start, job.rows)
            H[job.layer + 1, at:at + cut] = jnp.where(first, jnp.zeros((cut, CH), BF16), new[:cut])
            if cut < job.rows:
                H[job.layer + 1, at + cut:at + job.rows] = new[cut:]
        else:
            H[job.layer + 1, at:at + job.rows] = new
        finished.add(n)

    def add_skip(rows, part):
        S[rows] = S[rows] + part if rows.start // TILE in summed else part

    def skip_stage(layer, count, start):
        for low in (start, start + TILE):
            rows = slice(low, low + TILE)
            add_skip(rows, dot(G[rows, layer * CH:(layer + count) * CH], WS[layer * CH:(layer + count) * CH]))
            summed.add(low // TILE)

    pipe = []

    def retire():
        n, g = pipe.pop()
        fin_stage(n, g)

    load_x.wait()
    load_b.wait()
    for at, step in enumerate(steps):
        if step[0] == "S":
            assert "skip" in weighed
            skip_stage(*step[1])
            continue
        if step[0] == "J":
            n = step[1]
            assert finished.issuperset(jobs[n].needs), jobs[n]
            wait_for(n)
            g = gate_stage(jobs[n], z_stage(jobs[n]))
            gated.add(n)
        if pipe:
            retire()
        if step[-1]:
            send(step[-1])
            for k in [k[1] for k in steps[at + 1:at + 2] if k[0] == "J"]:
                wait_for(k)
        if step[0] == "J":
            pipe.append((n, g))
    if pipe:
        retire()

    @pl.when(me < devices - 1)
    def _():
        for h in halos:
            remote(h).wait_send()


def head_kernel(S, h, w1, b1, w2, b2, y, h_out, Y, sem):
    pass_h = pltpu.make_async_copy(h, h_out, sem.at[0])
    pass_h.start()
    writes = []
    for n, start in enumerate(range(0, ROWS, HEAD_ROWS)):
        rows = slice(start, start + HEAD_ROWS)
        a = jnp.maximum(S[rows], 0.0).astype(BF16)
        m = jnp.maximum(dot(a, w1[...]) + b1[...], 0.0).astype(BF16)
        Y[rows] = dot(m, w2[...]) + b2[...]
        c = pltpu.make_async_copy(Y.at[rows], y.at[rows], sem.at[1 + n])
        c.start()
        writes.append(c)
    pass_h.wait()
    for c in writes:
        c.wait()


def solution(mesh):
    devices = mesh.shape["sp"]
    jobs, halos, steps = plan()
    tall = {h.layer: max(-k.start for k in halos if k.layer == h.layer) for h in halos}
    rows = P(("ens", "sp"), None)

    def local(x, wp, wn, b, wr, ws, w1, b1, w2, b2):
        hbm, near = pl.BlockSpec(memory_space=pltpu.HBM), pl.BlockSpec(memory_space=pltpu.VMEM)
        vmem = lambda *shape: pltpu.VMEM(shape, BF16)
        skip, hidden = pl.pallas_call(
            lambda *refs: stack_kernel(jobs, halos, steps, devices, *refs),
            out_shape=(pltpu.VMEM((ROWS, CH), F32), pltpu.VMEM((ROWS, CH), BF16)),
            in_specs=[hbm] * 6,
            out_specs=(near, near),
            scratch_shapes=[
                vmem(LAYERS, HALO + ROWS, CH), vmem(ROWS, (LAYERS - 1) * CH),
                vmem(LAYERS, 2 * CH, 2 * CH), vmem(LAYERS, CH, CH), vmem(LAYERS * CH, CH),
                pltpu.VMEM((CYCLE, LAYERS // CYCLE, 2 * CH), F32),
                pltpu.SemaphoreType.DMA((LAYERS + 3,)),
                pltpu.SemaphoreType.DMA((len(halos),)), pltpu.SemaphoreType.DMA((len(halos),)),
            ] + [vmem(n, CH) for n in tall.values()],
            compiler_params=pltpu.CompilerParams(collective_id=0, has_side_effects=True, vmem_limit_bytes=56 * 1024 * 1024),
            name="wavenet_stack",
        )(x, wp.reshape(LAYERS, CH, 2 * CH), wn.reshape(LAYERS, CH, 2 * CH), jnp.swapaxes(b, 0, 1),
          wr.reshape(LAYERS, CH, CH), ws.reshape(LAYERS * CH, CH))
        return pl.pallas_call(
            head_kernel,
            out_shape=(jax.ShapeDtypeStruct((ROWS, CH), F32), jax.ShapeDtypeStruct((ROWS, CH), BF16)),
            in_specs=[near] * 6,
            out_specs=(hbm, hbm),
            scratch_shapes=[pltpu.VMEM((ROWS, CH), F32), pltpu.SemaphoreType.DMA((1 + ROWS // HEAD_ROWS,))],
            compiler_params=pltpu.CompilerParams(vmem_limit_bytes=6 * 1024 * 1024),
            name="wavenet_head",
        )(skip, hidden, w1, b1.reshape(1, CH), w2, b2.reshape(1, CH))

    return jax.shard_map(local, mesh=mesh, in_specs=(rows,) + (P(),) * 9, out_specs=(rows, rows), check_vma=False)
```
